16 devices in a mesh: dp: 2 (over z), fsdp: 8 (over y, x, core).
Axes of the slice: x: 2, y: 2, z: 2, core: 2. Of those that a mesh axis runs over, the one named last changes fastest.
Arguments:
- hidden: bfloat16 [16, 1024, 960], P(('dp', 'fsdp'))
- cot_out: bfloat16 [16, 1024, 960], P(('dp', 'fsdp'))
- attn_norm: bfloat16 [2, 960], P(None, 'fsdp')
- w_query: bfloat16 [2, 960, 15, 64], P(None, 'fsdp')
- w_key: bfloat16 [2, 960, 5, 64], P(None, 'fsdp')
- w_value: bfloat16 [2, 960, 5, 64], P(None, 'fsdp')
- w_out: bfloat16 [2, 960, 960], P(None, 'fsdp')
- mlp_norm: bfloat16 [2, 960], P(None, 'fsdp')
- w_gate: bfloat16 [2, 960, 2560], P(None, 'fsdp')
- w_up: bfloat16 [2, 960, 2560], P(None, 'fsdp')
- w_down: bfloat16 [2, 2560, 960], P(None, 'fsdp')
Outputs:
- output 1: bfloat16 [16, 1024, 960], P(('dp', 'fsdp'))
- output 2: bfloat16 [16, 1024, 960], P(('dp', 'fsdp'))
- output 3: float32 [2, 960], P(None, 'fsdp')
- output 4: float32 [2, 960, 15, 64], P(None, 'fsdp')
- output 5: float32 [2, 960, 5, 64], P(None, 'fsdp')
- output 6: float32 [2, 960, 5, 64], P(None, 'fsdp')
- output 7: float32 [2, 960, 960], P(None, 'fsdp')
- output 8: float32 [2, 960], P(None, 'fsdp')
- output 9: float32 [2, 960, 2560], P(None, 'fsdp')
- output 10: float32 [2, 960, 2560], P(None, 'fsdp')
- output 11: float32 [2, 2560, 960], P(None, 'fsdp')
All inputs are finite; a program needn't handle non-finite values.
Results may differ from the reference program's by a relative error of at most 0.02.
Values are sent between devices in bfloat16 or wider.
A program may use at most 1 GiB of HBM per device.

```python
import functools
import math
import jax
import jax.numpy as jnp
from jax import lax

D = 960
HEADS = 15
KV_HEADS = 5
HEAD = 64
FF = 2560
BATCH = 16
SEQ = 1024
LAYERS = 2

NORM_EPS = 1e-5
ROPE_THETA = 500000.0
ROPE_FACTOR = 8.0
LOW_FACTOR = 1.0
HIGH_FACTOR = 4.0
OLD_CONTEXT = 8192.0


def setup_inputs(seed: int = 0) -> dict:
    root_key = jax.random.key(seed)
    sub_keys = jax.random.split(root_key, 11)
    hidden = jax.random.normal(sub_keys[0], (BATCH, SEQ, D), jnp.float32).astype(jnp.bfloat16)
    cot_out = jax.random.normal(sub_keys[1], (BATCH, SEQ, D), jnp.float32).astype(jnp.bfloat16)
    attn_norm = (1.0 + 0.2 * jax.random.normal(sub_keys[2], (LAYERS, D), jnp.float32)).astype(jnp.bfloat16)
    w_query = (jax.random.normal(sub_keys[3], (LAYERS, D, HEADS, HEAD), jnp.float32) * D ** -0.5).astype(jnp.bfloat16)
    w_key = (jax.random.normal(sub_keys[4], (LAYERS, D, KV_HEADS, HEAD), jnp.float32) * D ** -0.5).astype(jnp.bfloat16)
    w_value = (jax.random.normal(sub_keys[5], (LAYERS, D, KV_HEADS, HEAD), jnp.float32) * D ** -0.5).astype(jnp.bfloat16)
    w_out = (jax.random.normal(sub_keys[6], (LAYERS, HEADS * HEAD, D), jnp.float32) * (HEADS * HEAD) ** -0.5).astype(jnp.bfloat16)
    mlp_norm = (1.0 + 0.2 * jax.random.normal(sub_keys[7], (LAYERS, D), jnp.float32)).astype(jnp.bfloat16)
    w_gate = (jax.random.normal(sub_keys[8], (LAYERS, D, FF), jnp.float32) * D ** -0.5).astype(jnp.bfloat16)
    w_up = (jax.random.normal(sub_keys[9], (LAYERS, D, FF), jnp.float32) * D ** -0.5).astype(jnp.bfloat16)
    w_down = (jax.random.normal(sub_keys[10], (LAYERS, FF, D), jnp.float32) * FF ** -0.5).astype(jnp.bfloat16)
    return {'hidden': hidden, 'cot_out': cot_out, 'attn_norm': attn_norm, 'w_query': w_query, 'w_key': w_key, 'w_value': w_value, 'w_out': w_out, 'mlp_norm': mlp_norm, 'w_gate': w_gate, 'w_up': w_up, 'w_down': w_down}


def rope_tables(seq_len, head_dim):
    half_dim = head_dim // 2
    base_freq = 1.0 / (ROPE_THETA ** (jnp.arange(half_dim, dtype=jnp.float32) * 2.0 / head_dim))
    wave_len = 2.0 * math.pi / base_freq
    smooth = (OLD_CONTEXT / wave_len - LOW_FACTOR) / (HIGH_FACTOR - LOW_FACTOR)
    mid_freq = (1.0 - smooth) * base_freq / ROPE_FACTOR + smooth * base_freq
    scaled_freq = jnp.where(wave_len < OLD_CONTEXT / HIGH_FACTOR, base_freq, jnp.where(wave_len > OLD_CONTEXT / LOW_FACTOR, base_freq / ROPE_FACTOR, mid_freq))
    angles = jnp.arange(seq_len, dtype=jnp.float32)[:, None] * scaled_freq[None, :]
    return jnp.cos(angles), jnp.sin(angles)


def rms_norm(act_f32, norm_gain):
    inv_rms = lax.rsqrt(jnp.mean(act_f32 * act_f32, axis=-1, keepdims=True) + NORM_EPS)
    return (act_f32 * inv_rms * norm_gain).astype(jnp.bfloat16)


def apply_rope(act_f32, cos_t, sin_t):
    half_dim = act_f32.shape[-1] // 2
    low_half = act_f32[..., :half_dim]
    high_half = act_f32[..., half_dim:]
    cos_b = cos_t[:, None, :]
    sin_b = sin_t[:, None, :]
    return jnp.concatenate([low_half * cos_b - high_half * sin_b, high_half * cos_b + low_half * sin_b], axis=-1)


def attend_one(seq_parts, cos_t, sin_t):
    query_s, key_s, value_s = seq_parts
    query_rot = apply_rope(query_s, cos_t, sin_t).astype(jnp.bfloat16).astype(jnp.float32).reshape(SEQ, KV_HEADS, HEADS // KV_HEADS, HEAD)
    key_rot = apply_rope(key_s, cos_t, sin_t).astype(jnp.bfloat16).astype(jnp.float32)
    scores = jnp.einsum('skgd,tkd->kgst', query_rot, key_rot) * HEAD ** -0.5
    causal = jnp.arange(SEQ)[:, None] >= jnp.arange(SEQ)[None, :]
    scores = jnp.where(causal, scores, -1e30)
    attn_probs = jax.nn.softmax(scores, axis=-1).astype(jnp.bfloat16).astype(jnp.float32)
    attn_mix = jnp.einsum('kgst,tkd->skgd', attn_probs, value_s)
    return attn_mix.astype(jnp.bfloat16).astype(jnp.float32).reshape(SEQ, HEADS * HEAD)


def layer_forward(hidden, params, cos_t, sin_t):
    attn_gain, w_query, w_key, w_value, w_out, mlp_gain, w_gate, w_up, w_down = params
    hid_f32 = hidden.astype(jnp.float32)
    normed = rms_norm(hid_f32, attn_gain).astype(jnp.float32).reshape(BATCH * SEQ, D)
    query_f = jnp.dot(normed, w_query.reshape(D, HEADS * HEAD), preferred_element_type=jnp.float32).reshape(BATCH, SEQ, HEADS, HEAD)
    key_f = jnp.dot(normed, w_key.reshape(D, KV_HEADS * HEAD), preferred_element_type=jnp.float32).reshape(BATCH, SEQ, KV_HEADS, HEAD)
    value_f = jnp.dot(normed, w_value.reshape(D, KV_HEADS * HEAD), preferred_element_type=jnp.float32).astype(jnp.bfloat16).astype(jnp.float32).reshape(BATCH, SEQ, KV_HEADS, HEAD)
    attn_fn = jax.checkpoint(functools.partial(attend_one, cos_t=cos_t, sin_t=sin_t))
    attn_out = lax.map(attn_fn, (query_f, key_f, value_f)).reshape(BATCH * SEQ, HEADS * HEAD)
    mid_hidden = (hid_f32 + jnp.dot(attn_out, w_out, preferred_element_type=jnp.float32).reshape(BATCH, SEQ, D)).astype(jnp.bfloat16)
    mid_f32 = mid_hidden.astype(jnp.float32)
    normed_mlp = rms_norm(mid_f32, mlp_gain).astype(jnp.float32).reshape(BATCH * SEQ, D)
    gate_proj = jnp.dot(normed_mlp, w_gate, preferred_element_type=jnp.float32)
    up_proj = jnp.dot(normed_mlp, w_up, preferred_element_type=jnp.float32)
    mlp_act = (jax.nn.silu(gate_proj) * up_proj).astype(jnp.bfloat16).astype(jnp.float32)
    return (mid_f32 + jnp.dot(mlp_act, w_down, preferred_element_type=jnp.float32).reshape(BATCH, SEQ, D)).astype(jnp.bfloat16)


def reference(hidden, cot_out, attn_norm, w_query, w_key, w_value, w_out, mlp_norm, w_gate, w_up, w_down):
    cos_t, sin_t = rope_tables(SEQ, HEAD)
    weights_f32 = (attn_norm.astype(jnp.float32), w_query.astype(jnp.float32), w_key.astype(jnp.float32), w_value.astype(jnp.float32), w_out.astype(jnp.float32), mlp_norm.astype(jnp.float32), w_gate.astype(jnp.float32), w_up.astype(jnp.float32), w_down.astype(jnp.float32))

    def run_layers(hidden_in, weight_stack):
        def scan_body(carry_hidden, layer_params):
            return layer_forward(carry_hidden, layer_params, cos_t, sin_t), None
        hidden_out, _unused = lax.scan(scan_body, hidden_in, weight_stack)
        return hidden_out

    out_hidden, pullback = jax.vjp(run_layers, hidden, weights_f32)
    grad_hidden, grad_weights = pullback(cot_out)
    grad_scale = 1.0 / (BATCH * SEQ)
    return (out_hidden, grad_hidden, grad_weights[0] * grad_scale, grad_weights[1] * grad_scale, grad_weights[2] * grad_scale, grad_weights[3] * grad_scale, grad_weights[4] * grad_scale, grad_weights[5] * grad_scale, grad_weights[6] * grad_scale, grad_weights[7] * grad_scale, grad_weights[8] * grad_scale)
```

```python
import functools
import math
import jax
import jax.numpy as jnp
from jax import lax
from jax.experimental import pallas as pl
from jax.experimental.layout import Layout, with_layout_constraint
from jax.experimental.pallas import tpu as pltpu
from jax.sharding import PartitionSpec as P

NORM_EPS = 1e-5
ROPE_THETA = 500000.0
ROPE_FACTOR = 8.0
LOW_FACTOR = 1.0
HIGH_FACTOR = 4.0
OLD_CONTEXT = 8192.0
F32 = jnp.float32
BF16 = jnp.bfloat16
D, HEADS, KV, HD, FF = 960, 15, 5, 64, 2560
GROUP = HEADS // KV
BLK = 256
TOKEN_SPEC = P(('dp', 'fsdp'), None, None)
WEIGHT_SPECS = (P(None, 'fsdp'), P(None, 'fsdp', None, None), P(None, 'fsdp', None, None), P(None, 'fsdp', None, None), P(None, 'fsdp', None), P(None, 'fsdp'), P(None, 'fsdp', None), P(None, 'fsdp', None), P(None, 'fsdp', None))
CORE_SWAP = [(i, i ^ 1) for i in range(8)]
DP_SWAP = [(0, 1), (1, 0)]
SAME_CORE = [[0, 2, 4, 6], [1, 3, 5, 7]]
LOG2E = 1.4426950408889634
SCALE = HD ** -0.5


def rope_tables(seq_len, head_dim):
    half_dim = head_dim // 2
    base_freq = 1.0 / (ROPE_THETA ** (jnp.arange(half_dim, dtype=jnp.float32) * 2.0 / head_dim))
    wave_len = 2.0 * math.pi / base_freq
    smooth = (OLD_CONTEXT / wave_len - LOW_FACTOR) / (HIGH_FACTOR - LOW_FACTOR)
    mid_freq = (1.0 - smooth) * base_freq / ROPE_FACTOR + smooth * base_freq
    scaled_freq = jnp.where(wave_len < OLD_CONTEXT / HIGH_FACTOR, base_freq, jnp.where(wave_len > OLD_CONTEXT / LOW_FACTOR, base_freq / ROPE_FACTOR, mid_freq))
    angles = jnp.arange(seq_len, dtype=jnp.float32)[None, :] * scaled_freq[:, None]
    return jnp.cos(angles), jnp.sin(angles)


def dot_nn(a, b):
    return lax.dot_general(a, b, (((1,), (0,)), ((), ())), preferred_element_type=F32)


def dot_nt(a, b):
    return lax.dot_general(a, b, (((1,), (1,)), ((), ())), preferred_element_type=F32)


def dot_tn(a, b):
    return lax.dot_general(a, b, (((0,), (0,)), ((), ())), preferred_element_type=F32)


def rotate(x, cos, sin):
    u, w = x[:HD // 2], x[HD // 2:]
    return jnp.concatenate([u * cos - w * sin, w * cos + u * sin], axis=0)


def unrotate(x, cos, sin):
    u, w = x[:HD // 2], x[HD // 2:]
    return jnp.concatenate([u * cos + w * sin, w * cos - u * sin], axis=0)


def score_parts(k_ref, q, i):
    parts = []
    if i:
        parts.append(dot_nn(k_ref[:i * BLK], q))
    diag = dot_nn(k_ref[i * BLK:(i + 1) * BLK], q)
    keys = lax.broadcasted_iota(jnp.int32, (BLK, BLK), 0)
    queries = lax.broadcasted_iota(jnp.int32, (BLK, BLK), 1)
    parts.append(jnp.where(keys <= queries, diag, -1e30 / SCALE))
    return parts


def softmax_parts(parts):
    top = functools.reduce(jnp.maximum, [jnp.max(s, axis=0, keepdims=True) for s in parts])
    exps = [jnp.exp2((s - top) * (SCALE * LOG2E)) for s in parts]
    inv = 1.0 / sum(jnp.sum(e, axis=0, keepdims=True) for e in exps)
    return [e * inv for e in exps]


def attn_fwd_kernel(q_ref, k_ref, v_ref, cos_ref, sin_ref, qr_ref, kr_ref, vb_ref, o_ref, kt_ref):
    cos, sin = cos_ref[...], sin_ref[...]
    kr = rotate(k_ref[...], cos, sin).astype(BF16)
    kr_ref[...] = kr
    kt_ref[...] = jnp.transpose(kr.astype(F32)).astype(BF16)
    vb_ref[...] = v_ref[...].astype(BF16)

    def head(h, carry):
        rows = pl.ds(pl.multiple_of(h * HD, HD), HD)
        qr_ref[rows, :] = rotate(q_ref[rows, :], cos, sin).astype(BF16)
        for i in range(q_ref.shape[1] // BLK):
            cols = slice(i * BLK, (i + 1) * BLK)
            probs = softmax_parts(score_parts(kt_ref, qr_ref[rows, cols], i))
            base = 0
            out = None
            for p in probs:
                term = dot_nn(vb_ref[:, base:base + p.shape[0]], p.astype(BF16))
                out = term if out is None else out + term
                base += p.shape[0]
            o_ref[rows, cols] = out.astype(BF16)
        return carry

    lax.fori_loop(0, GROUP, head, 0)


def attn_bwd_kernel(q_ref, k_ref, v_ref, do_ref, cos_ref, sin_ref, dq_ref, dk_ref, dv_ref, kt_ref, vt_ref, dka_ref, dva_ref):
    cos, sin = cos_ref[...], sin_ref[...]
    kt_ref[...] = jnp.transpose(k_ref[...].astype(F32)).astype(BF16)
    vt_ref[...] = jnp.transpose(v_ref[...].astype(F32)).astype(BF16)
    dka_ref[...] = jnp.zeros_like(dka_ref)
    dva_ref[...] = jnp.zeros_like(dva_ref)

    def head(h, carry):
        rows = pl.ds(pl.multiple_of(h * HD, HD), HD)
        for i in range(q_ref.shape[1] // BLK):
            cols = slice(i * BLK, (i + 1) * BLK)
            q, do = q_ref[rows, cols], do_ref[rows, cols]
            probs = softmax_parts(score_parts(kt_ref, q, i))
            base = 0
            dps = []
            for p in probs:
                keys = slice(base, base + p.shape[0])
                dps.append(dot_nn(vt_ref[keys], do).astype(BF16).astype(F32))
                dva_ref[keys] += dot_nt(p.astype(BF16), do)
                base += p.shape[0]
            mean = sum(jnp.sum(p * dp, axis=0, keepdims=True) for p, dp in zip(probs, dps))
            base = 0
            dq = None
            for p, dp in zip(probs, dps):
                keys = slice(base, base + p.shape[0])
                ds = (p * (dp - mean)).astype(BF16)
                dka_ref[keys] += dot_nt(ds, q)
                term = dot_nn(k_ref[:, keys], ds)
                dq = term if dq is None else dq + term
                base += p.shape[0]
            dq = (dq * SCALE).astype(BF16).astype(F32)
            dq_ref[rows, cols] = unrotate(dq, cos[:, cols], sin[:, cols]).astype(BF16)
        return carry

    lax.fori_loop(0, GROUP, head, 0)
    dk = (jnp.transpose(dka_ref[...]) * SCALE).astype(BF16).astype(F32)
    dk_ref[...] = unrotate(dk, cos, sin).astype(BF16)
    dv_ref[...] = jnp.transpose(dva_ref[...]).astype(BF16)


def head_spec(seq, first, size):
    return pl.BlockSpec((size, seq), lambda g: (first + g, 0))


def attention_forward(qkv, cos, sin):
    seq = qkv.shape[1]
    full = pl.BlockSpec((HD // 2, seq), lambda g: (0, 0))
    shape = lambda rows: jax.ShapeDtypeStruct((rows, seq), BF16)
    return pl.pallas_call(
        attn_fwd_kernel,
        grid=(KV,),
        in_specs=[head_spec(seq, 0, GROUP * HD), head_spec(seq, HEADS, HD), head_spec(seq, HEADS + KV, HD), full, full],
        out_specs=[head_spec(seq, 0, GROUP * HD), head_spec(seq, 0, HD), head_spec(seq, 0, HD), head_spec(seq, 0, GROUP * HD)],
        out_shape=[shape(HEADS * HD), shape(KV * HD), shape(KV * HD), shape(HEADS * HD)],
        scratch_shapes=[pltpu.VMEM((seq, HD), BF16)],
        compiler_params=pltpu.CompilerParams(dimension_semantics=('arbitrary',), vmem_limit_bytes=48 * 1024 * 1024),
        cost_estimate=pl.CostEstimate(flops=20_000_000_000, bytes_accessed=14_000_000, transcendentals=10_000_000),
        name='attn_fwd',
    )(qkv, qkv, qkv, cos, sin)


def attention_backward(qr, kr, vb, do, cos, sin):
    seq = qr.shape[1]
    full = pl.BlockSpec((HD // 2, seq), lambda g: (0, 0))
    shape = lambda rows: jax.ShapeDtypeStruct((rows, seq), BF16)
    return pl.pallas_call(
        attn_bwd_kernel,
        grid=(KV,),
        in_specs=[head_spec(seq, 0, GROUP * HD), head_spec(seq, 0, HD), head_spec(seq, 0, HD), head_spec(seq, 0, GROUP * HD), full, full],
        out_specs=[head_spec(seq, 0, GROUP * HD), head_spec(seq, 0, HD), head_spec(seq, 0, HD)],
        out_shape=[shape(HEADS * HD), shape(KV * HD), shape(KV * HD)],
        scratch_shapes=[pltpu.VMEM((seq, HD), BF16), pltpu.VMEM((seq, HD), BF16), pltpu.VMEM((seq, HD), F32), pltpu.VMEM((seq, HD), F32)],
        compiler_params=pltpu.CompilerParams(dimension_semantics=('arbitrary',), vmem_limit_bytes=48 * 1024 * 1024),
        cost_estimate=pl.CostEstimate(flops=40_000_000_000, bytes_accessed=14_000_000, transcendentals=10_000_000),
        name='attn_bwd',
    )(qr, kr, vb, do, cos, sin)


def mlp_bwd_kernel(down_ref, grad_ref, gate_ref, up_ref, out_ref):
    dact = dot_nn(down_ref[...], grad_ref[...]).astype(BF16).astype(F32)
    gate, up = gate_ref[...], up_ref[...]
    sig = jax.nn.sigmoid(gate)
    out_ref[0] = (dact * up * (sig * (1.0 + gate * (1.0 - sig)))).astype(BF16)
    out_ref[1] = (dact * (gate * sig)).astype(BF16)


def mlp_backward(down, grad, gate, up):
    seq = grad.shape[1]
    rows = pl.BlockSpec((256, seq), lambda i: (i, 0))
    out = pl.pallas_call(
        mlp_bwd_kernel,
        grid=(FF // 256,),
        in_specs=[pl.BlockSpec((256, D), lambda i: (i, 0)), pl.BlockSpec((D, seq), lambda i: (0, 0)), rows, rows],
        out_specs=pl.BlockSpec((2, 256, seq), lambda i: (0, i, 0)),
        out_shape=jax.ShapeDtypeStruct((2, FF, seq), BF16),
        compiler_params=pltpu.CompilerParams(dimension_semantics=('arbitrary',), vmem_limit_bytes=32 * 1024 * 1024),
        cost_estimate=pl.CostEstimate(flops=5_000_000_000, bytes_accessed=38_000_000, transcendentals=5_000_000),
        name='mlp_bwd',
    )(down, grad, gate, up)
    return out.reshape(2 * FF, seq)


def rms_forward(x, gain):
    inv = lax.rsqrt(jnp.mean(x * x, axis=0, keepdims=True) + NORM_EPS)
    return (x * inv * gain).astype(BF16), inv


def rms_backward(x, inv, gain, dn):
    dgain = jnp.sum(dn * (x * inv), axis=1)
    dxn = dn * gain
    dot = jnp.sum(dxn * x, axis=0, keepdims=True)
    return dxn * inv - x * (inv * inv * inv * dot * (1.0 / x.shape[0])), dgain


def core_half(a, core):
    rows = a.shape[0] // 8
    blocks = a.reshape(4, 2, rows, a.shape[1])
    return lax.dynamic_index_in_dim(blocks, core, axis=1, keepdims=False).reshape(4 * rows, a.shape[1])


def to_peer(part):
    return lax.ppermute(part, 'fsdp', CORE_SWAP)


def row_major(a):
    return with_layout_constraint(a, Layout(major_to_minor=(0, 1)))


def over_chips(part):
    return lax.psum_scatter(part, 'fsdp', scatter_dimension=0, tiled=True, axis_index_groups=SAME_CORE)


def over_dp(mine):
    peer = lax.ppermute(mine, 'dp', DP_SWAP)
    return mine + peer


def tie(*values):
    return lax.optimization_barrier(values)


def gather(shard):
    return lax.all_gather(shard, 'fsdp', axis=0, tiled=True)


def solution(mesh):
    device_count = mesh.shape['dp'] * mesh.shape['fsdp']

    def local_step(hidden, cot_out, attn_norm, w_query, w_key, w_value, w_out, mlp_norm, w_gate, w_up, w_down):
        layers = attn_norm.shape[0]
        rows = attn_norm.shape[1]
        seq = hidden.shape[1]
        core = lax.rem(lax.axis_index('fsdp'), 2)
        cos, sin = rope_tables(seq, HD)
        grad_scale = 1.0 / (seq * device_count)
        gains = jnp.stack([attn_norm[0], mlp_norm[0], attn_norm[1], mlp_norm[1]], axis=1)
        gains = jnp.pad(gains, ((0, 0), (0, 124)))
        weights = []
        for l in range(layers):
            pieces = [w_query[l].reshape(rows, HEADS * HD), w_key[l].reshape(rows, KV * HD), w_value[l].reshape(rows, KV * HD), w_out[l]]
            if l == 0:
                pieces.append(gains)
            attn_w = gather(jnp.concatenate(pieces, axis=1))
            gate_up = gather(jnp.concatenate([w_gate[l], w_up[l]], axis=1))
            down = gather(w_down[l])
            weights.append((attn_w, gate_up, down))
        gain_cols = weights[0][0][:, 2560:2564].astype(F32)
        x = hidden[0].T
        saved = []
        for l in range(layers):
            attn_w, gate_up, down = weights[l]
            g1, g2 = gain_cols[:, 2 * l:2 * l + 1], gain_cols[:, 2 * l + 1:2 * l + 2]
            xf = x.astype(F32)
            a, inv1 = rms_forward(xf, g1)
            qkv = dot_tn(attn_w[:, :1600], a)
            qr, kr, vb, o = attention_forward(qkv, cos, sin)
            x1 = (xf + dot_tn(attn_w[:, 1600:2560], o)).astype(BF16)
            x1f = x1.astype(F32)
            b, inv2 = rms_forward(x1f, g2)
            gate = dot_tn(gate_up[:, :FF], b)
            up = dot_tn(gate_up[:, FF:], b)
            act = (jax.nn.silu(gate) * up).astype(BF16)
            saved.append((x, a, inv1, g1, qr, kr, vb, o, x1, b, inv2, g2, gate, up, act))
            x = (x1f + dot_tn(down, act)).astype(BF16)
        y = x
        grad = cot_out[0].T
        outs = [[None] * 3 for _ in range(layers)]
        gain_grads = [None] * (2 * layers)
        waiting = []

        def release(value):
            if not waiting:
                return value
            l, slot, part = waiting.pop(0)
            value, part = tie(value, part)
            outs[l][slot] = over_dp(part)
            return value

        for l in reversed(range(layers)):
            attn_w, gate_up, down = weights[l]
            x, a, inv1, g1, qr, kr, vb, o, x1, b, inv2, g2, gate, up, act = saved[l]
            wide = jnp.pad(grad, ((0, 64), (0, 0)))
            other_down = row_major(dot_nt(core_half(act, 1 - core), wide))
            grad, other_down = tie(grad, other_down)
            sent_down = to_peer(other_down)
            dgu = mlp_backward(down, grad, gate, up)
            act_mine, dgu = tie(core_half(act, core), dgu)
            mine_down = row_major(dot_nt(act_mine, wide) + sent_down)
            other_gu = row_major(dot_nt(core_half(b, 1 - core), dgu))
            dgu, mine_down, other_gu = tie(dgu, mine_down, other_gu)
            waiting.append((l, 2, over_chips(mine_down)))
            sent_gu = to_peer(other_gu)
            db = dot_nn(gate_up, dgu).astype(BF16).astype(F32)
            dx1n, gain_grads[2 * l + 1] = rms_backward(x1.astype(F32), inv2, g2, db)
            dmid = (grad.astype(F32) + dx1n).astype(BF16)
            if l == 0:
                dmid = release(dmid)
            b_mine, dmid = tie(core_half(b, core), dmid)
            mine_gu = row_major(dot_nt(b_mine, dgu) + sent_gu)
            other_o = row_major(dot_nt(core_half(o, 1 - core), dmid))
            dmid, mine_gu, other_o = tie(dmid, mine_gu, other_o)
            waiting.append((l, 1, over_chips(mine_gu)))
            sent_o = to_peer(other_o)
            do = dot_nn(attn_w[:, 1600:2560], dmid).astype(BF16)
            dq, dk, dv = attention_backward(qr, kr, vb, do, cos, sin)
            dqkv = release(jnp.concatenate([dq, dk, dv], axis=0))
            o_mine, dqkv = tie(core_half(o, core), dqkv)
            mine_o = dot_nt(o_mine, dmid) + sent_o
            other_qkv = row_major(dot_nt(core_half(a, 1 - core), dqkv))
            dqkv, mine_o, other_qkv = tie(dqkv, mine_o, other_qkv)
            sent_qkv = to_peer(other_qkv)
            da = dot_nn(attn_w[:, :1600], dqkv).astype(BF16).astype(F32)
            dxn, gain_grads[2 * l] = rms_backward(x.astype(F32), inv1, g1, da)
            grad = (dmid.astype(F32) + dxn).astype(BF16)
            a_mine, grad = tie(core_half(a, core), grad)
            parts = [dot_nt(a_mine, dqkv) + sent_qkv, mine_o]
            if l == 0:
                cols = jnp.pad(jnp.stack(gain_grads, axis=1), ((0, 0), (0, 124)))
                parts.append(core_half(cols, core) + to_peer(core_half(cols, 1 - core)))
            part = row_major(jnp.concatenate(parts, axis=1))
            grad, part = tie(grad, part)
            if l == 0:
                part = release(release(part))
            waiting.append((l, 0, over_chips(part)))
        for l, slot, part in waiting:
            outs[l][slot] = over_dp(part)
        ra = [o[0] * grad_scale for o in outs]
        rg = [o[1] * grad_scale for o in outs]
        rd = [o[2][:, :D] * grad_scale for o in outs]
        gain = ra[0][:, 2560:2564]
        stack = lambda parts: jnp.stack(parts)
        return (
            y.T[None], grad.T[None],
            stack([gain[:, 0], gain[:, 2]]),
            stack([r[:, :960].reshape(rows, HEADS, HD) for r in ra]),
            stack([r[:, 960:1280].reshape(rows, KV, HD) for r in ra]),
            stack([r[:, 1280:1600].reshape(rows, KV, HD) for r in ra]),
            stack([r[:, 1600:2560] for r in ra]),
            stack([gain[:, 1], gain[:, 3]]),
            stack([r[:, :FF] for r in rg]),
            stack([r[:, FF:] for r in rg]),
            stack(rd),
        )

    return jax.shard_map(local_step, mesh=mesh, in_specs=(TOKEN_SPEC, TOKEN_SPEC) + WEIGHT_SPECS, out_specs=(TOKEN_SPEC, TOKEN_SPEC) + WEIGHT_SPECS, check_vma=False)
```

```python
import functools
import math
import jax
import jax.numpy as jnp
from jax import lax
from jax.experimental import pallas as pl
from jax.experimental.layout import Layout, with_layout_constraint
from jax.experimental.pallas import tpu as pltpu
from jax.sharding import PartitionSpec as P

NORM_EPS = 1e-5
ROPE_THETA = 500000.0
ROPE_FACTOR = 8.0
LOW_FACTOR = 1.0
HIGH_FACTOR = 4.0
OLD_CONTEXT = 8192.0
F32 = jnp.float32
BF16 = jnp.bfloat16
D, HEADS, KV, HD, FF = 960, 15, 5, 64, 2560
GROUP = HEADS // KV
BLK = 256
WEST = 1408
TOKEN_SPEC = P(('dp', 'fsdp'), None, None)
WEIGHT_SPECS = (P(None, 'fsdp'), P(None, 'fsdp', None, None), P(None, 'fsdp', None, None), P(None, 'fsdp', None, None), P(None, 'fsdp', None), P(None, 'fsdp'), P(None, 'fsdp', None), P(None, 'fsdp', None), P(None, 'fsdp', None))
CORE_SWAP = [(i, i ^ 1) for i in range(8)]
DP_SWAP = [(0, 1), (1, 0)]
SAME_CORE = [[0, 2, 4, 6], [1, 3, 5, 7]]
LOG2E = 1.4426950408889634
SCALE = HD ** -0.5


def rope_tables(seq_len, head_dim):
    half_dim = head_dim // 2
    base_freq = 1.0 / (ROPE_THETA ** (jnp.arange(half_dim, dtype=jnp.float32) * 2.0 / head_dim))
    wave_len = 2.0 * math.pi / base_freq
    smooth = (OLD_CONTEXT / wave_len - LOW_FACTOR) / (HIGH_FACTOR - LOW_FACTOR)
    mid_freq = (1.0 - smooth) * base_freq / ROPE_FACTOR + smooth * base_freq
    scaled_freq = jnp.where(wave_len < OLD_CONTEXT / HIGH_FACTOR, base_freq, jnp.where(wave_len > OLD_CONTEXT / LOW_FACTOR, base_freq / ROPE_FACTOR, mid_freq))
    angles = jnp.arange(seq_len, dtype=jnp.float32)[None, :] * scaled_freq[:, None]
    return jnp.cos(angles), jnp.sin(angles)


def dot_nn(a, b):
    return lax.dot_general(a, b, (((1,), (0,)), ((), ())), preferred_element_type=F32)


def dot_nt(a, b):
    return lax.dot_general(a, b, (((1,), (1,)), ((), ())), preferred_element_type=F32)


def dot_tn(a, b):
    return lax.dot_general(a, b, (((0,), (0,)), ((), ())), preferred_element_type=F32)


def rotate(x, cos, sin):
    u, w = x[:HD // 2], x[HD // 2:]
    return jnp.concatenate([u * cos - w * sin, w * cos + u * sin], axis=0)


def unrotate(x, cos, sin):
    u, w = x[:HD // 2], x[HD // 2:]
    return jnp.concatenate([u * cos + w * sin, w * cos - u * sin], axis=0)


def score_parts(k_ref, q, i):
    parts = []
    if i:
        parts.append(dot_nn(k_ref[:i * BLK], q))
    diag = dot_nn(k_ref[i * BLK:(i + 1) * BLK], q)
    keys = lax.broadcasted_iota(jnp.int32, (BLK, BLK), 0)
    queries = lax.broadcasted_iota(jnp.int32, (BLK, BLK), 1)
    parts.append(jnp.where(keys <= queries, diag, -1e30 / SCALE))
    return parts


def softmax_parts(parts):
    top = functools.reduce(jnp.maximum, [jnp.max(s, axis=0, keepdims=True) for s in parts])
    exps = [jnp.exp2((s - top) * (SCALE * LOG2E)) for s in parts]
    inv = 1.0 / sum(jnp.sum(e, axis=0, keepdims=True) for e in exps)
    return [e * inv for e in exps]


def attn_fwd_kernel(q_ref, k_ref, v_ref, cos_ref, sin_ref, qr_ref, kr_ref, vb_ref, o_ref, kt_ref):
    cos, sin = cos_ref[...], sin_ref[...]
    kr = rotate(k_ref[...], cos, sin).astype(BF16)
    kr_ref[...] = kr
    kt_ref[...] = jnp.transpose(kr.astype(F32)).astype(BF16)
    vb_ref[...] = v_ref[...].astype(BF16)

    def head(h, carry):
        rows = pl.ds(pl.multiple_of(h * HD, HD), HD)
        qr_ref[rows, :] = rotate(q_ref[rows, :], cos, sin).astype(BF16)
        for i in range(q_ref.shape[1] // BLK):
            cols = slice(i * BLK, (i + 1) * BLK)
            probs = softmax_parts(score_parts(kt_ref, qr_ref[rows, cols], i))
            base = 0
            out = None
            for p in probs:
                term = dot_nn(vb_ref[:, base:base + p.shape[0]], p.astype(BF16))
                out = term if out is None else out + term
                base += p.shape[0]
            o_ref[rows, cols] = out.astype(BF16)
        return carry

    lax.fori_loop(0, GROUP, head, 0)


def attn_bwd_kernel(q_ref, k_ref, v_ref, do_ref, cos_ref, sin_ref, dq_ref, dk_ref, dv_ref, kt_ref, vt_ref, dka_ref, dva_ref):
    cos, sin = cos_ref[...], sin_ref[...]
    kt_ref[...] = jnp.transpose(k_ref[...].astype(F32)).astype(BF16)
    vt_ref[...] = jnp.transpose(v_ref[...].astype(F32)).astype(BF16)
    dka_ref[...] = jnp.zeros_like(dka_ref)
    dva_ref[...] = jnp.zeros_like(dva_ref)

    def head(h, carry):
        rows = pl.ds(pl.multiple_of(h * HD, HD), HD)
        for i in range(q_ref.shape[1] // BLK):
            cols = slice(i * BLK, (i + 1) * BLK)
            q, do = q_ref[rows, cols], do_ref[rows, cols]
            probs = softmax_parts(score_parts(kt_ref, q, i))
            base = 0
            dps = []
            for p in probs:
                keys = slice(base, base + p.shape[0])
                dps.append(dot_nn(vt_ref[keys], do).astype(BF16).astype(F32))
                dva_ref[keys] += dot_nt(p.astype(BF16), do)
                base += p.shape[0]
            mean = sum(jnp.sum(p * dp, axis=0, keepdims=True) for p, dp in zip(probs, dps))
            base = 0
            dq = None
            for p, dp in zip(probs, dps):
                keys = slice(base, base + p.shape[0])
                ds = (p * (dp - mean)).astype(BF16)
                dka_ref[keys] += dot_nt(ds, q)
                term = dot_nn(k_ref[:, keys], ds)
                dq = term if dq is None else dq + term
                base += p.shape[0]
            dq = (dq * SCALE).astype(BF16).astype(F32)
            dq_ref[rows, cols] = unrotate(dq, cos[:, cols], sin[:, cols]).astype(BF16)
        return carry

    lax.fori_loop(0, GROUP, head, 0)
    dk = (jnp.transpose(dka_ref[...]) * SCALE).astype(BF16).astype(F32)
    dk_ref[...] = unrotate(dk, cos, sin).astype(BF16)
    dv_ref[...] = jnp.transpose(dva_ref[...]).astype(BF16)


def head_spec(seq, first, size):
    return pl.BlockSpec((size, seq), lambda g: (first + g, 0))


def attention_forward(qkv, cos, sin):
    seq = qkv.shape[1]
    full = pl.BlockSpec((HD // 2, seq), lambda g: (0, 0))
    shape = lambda rows: jax.ShapeDtypeStruct((rows, seq), BF16)
    return pl.pallas_call(
        attn_fwd_kernel,
        grid=(KV,),
        in_specs=[head_spec(seq, 0, GROUP * HD), head_spec(seq, HEADS, HD), head_spec(seq, HEADS + KV, HD), full, full],
        out_specs=[head_spec(seq, 0, GROUP * HD), head_spec(seq, 0, HD), head_spec(seq, 0, HD), head_spec(seq, 0, GROUP * HD)],
        out_shape=[shape(HEADS * HD), shape(KV * HD), shape(KV * HD), shape(HEADS * HD)],
        scratch_shapes=[pltpu.VMEM((seq, HD), BF16)],
        compiler_params=pltpu.CompilerParams(dimension_semantics=('arbitrary',), vmem_limit_bytes=48 * 1024 * 1024),
        cost_estimate=pl.CostEstimate(flops=20_000_000_000, bytes_accessed=14_000_000, transcendentals=10_000_000),
        name='attn_fwd',
    )(qkv, qkv, qkv, cos, sin)


def attention_backward(qr, kr, vb, do, cos, sin):
    seq = qr.shape[1]
    full = pl.BlockSpec((HD // 2, seq), lambda g: (0, 0))
    shape = lambda rows: jax.ShapeDtypeStruct((rows, seq), BF16)
    return pl.pallas_call(
        attn_bwd_kernel,
        grid=(KV,),
        in_specs=[head_spec(seq, 0, GROUP * HD), head_spec(seq, 0, HD), head_spec(seq, 0, HD), head_spec(seq, 0, GROUP * HD), full, full],
        out_specs=[head_spec(seq, 0, GROUP * HD), head_spec(seq, 0, HD), head_spec(seq, 0, HD)],
        out_shape=[shape(HEADS * HD), shape(KV * HD), shape(KV * HD)],
        scratch_shapes=[pltpu.VMEM((seq, HD), BF16), pltpu.VMEM((seq, HD), BF16), pltpu.VMEM((seq, HD), F32), pltpu.VMEM((seq, HD), F32)],
        compiler_params=pltpu.CompilerParams(dimension_semantics=('arbitrary',), vmem_limit_bytes=48 * 1024 * 1024),
        cost_estimate=pl.CostEstimate(flops=40_000_000_000, bytes_accessed=14_000_000, transcendentals=10_000_000),
        name='attn_bwd',
    )(qr, kr, vb, do, cos, sin)


def mlp_fwd_kernel(b_ref, wg_ref, wu_ref, gate_ref, up_ref, act_ref):
    gate = dot_tn(wg_ref[...], b_ref[...])
    up = dot_tn(wu_ref[...], b_ref[...])
    gate_ref[...] = gate
    up_ref[...] = up
    act_ref[...] = (gate * jax.nn.sigmoid(gate) * up).astype(BF16)


def mlp_forward(gate_up, b):
    seq = b.shape[1]
    steps = FF // 256
    rows = pl.BlockSpec((256, seq), lambda i: (i, 0))
    wide = jax.ShapeDtypeStruct((FF, seq), F32)
    return pl.pallas_call(
        mlp_fwd_kernel,
        grid=(steps,),
        in_specs=[pl.BlockSpec((D, seq), lambda i: (0, 0)), pl.BlockSpec((D, 256), lambda i: (0, i)), pl.BlockSpec((D, 256), lambda i: (0, steps + i))],
        out_specs=[rows, rows, rows],
        out_shape=[wide, wide, jax.ShapeDtypeStruct((FF, seq), BF16)],
        compiler_params=pltpu.CompilerParams(dimension_semantics=('arbitrary',), vmem_limit_bytes=32 * 1024 * 1024),
        cost_estimate=pl.CostEstimate(flops=10_000_000_000, bytes_accessed=38_000_000, transcendentals=5_000_000),
        name='mlp_fwd',
    )(b, gate_up, gate_up)


def mlp_bwd_kernel(down_ref, grad_ref, gate_ref, up_ref, out_ref):
    dact = dot_nn(down_ref[...], grad_ref[...]).astype(BF16).astype(F32)
    gate, up = gate_ref[...], up_ref[...]
    sig = jax.nn.sigmoid(gate)
    out_ref[0] = (dact * up * (sig * (1.0 + gate * (1.0 - sig)))).astype(BF16)
    out_ref[1] = (dact * (gate * sig)).astype(BF16)


def mlp_backward(down, grad, gate, up):
    seq = grad.shape[1]
    rows = pl.BlockSpec((256, seq), lambda i: (i, 0))
    out = pl.pallas_call(
        mlp_bwd_kernel,
        grid=(FF // 256,),
        in_specs=[pl.BlockSpec((256, D), lambda i: (i, 0)), pl.BlockSpec((D, seq), lambda i: (0, 0)), rows, rows],
        out_specs=pl.BlockSpec((2, 256, seq), lambda i: (0, i, 0)),
        out_shape=jax.ShapeDtypeStruct((2, FF, seq), BF16),
        compiler_params=pltpu.CompilerParams(dimension_semantics=('arbitrary',), vmem_limit_bytes=32 * 1024 * 1024),
        cost_estimate=pl.CostEstimate(flops=5_000_000_000, bytes_accessed=38_000_000, transcendentals=5_000_000),
        name='mlp_bwd',
    )(down, grad, gate, up)
    return out.reshape(2 * FF, seq)


def gather_kernel(shard_ref, out_ref, token_ref, send_sem, recv_sem):
    me = lax.axis_index('fsdp')
    over_c = me + 1 - 2 * (me % 2)
    over_x = me + 2 - 4 * ((me // 2) % 2)
    over_y = me + 4 - 8 * (me // 4)
    diag = over_x + over_y - me
    barrier = pltpu.get_barrier_semaphore()
    for peer in (over_x, over_y, over_c):
        pl.semaphore_signal(barrier, inc=1, device_id={'fsdp': peer}, device_id_type=pl.DeviceIdType.MESH)
    pl.semaphore_wait(barrier, 3)
    width = shard_ref.shape[1]
    left, right = pl.ds(0, WEST), pl.ds(WEST, width - WEST)

    def send(slot, src, dst, peer):
        copy = pltpu.make_async_remote_copy(
            src_ref=src, dst_ref=dst, send_sem=send_sem.at[slot], recv_sem=recv_sem.at[slot],
            device_id={'fsdp': peer}, device_id_type=pl.DeviceIdType.MESH)
        copy.start()
        return copy

    def relay(slot, shard, cols, peer):
        part = out_ref.at[shard, :, cols]
        return send(slot, part, part, peer)

    own_x = send(0, shard_ref, out_ref.at[me], over_x)
    own_y = send(1, shard_ref, out_ref.at[me], over_y)
    own_c = send(2, shard_ref, out_ref.at[me], over_c)
    out_ref[me] = shard_ref[...]
    token_ref[...] = jnp.zeros_like(token_ref)
    own_x.wait_recv()
    diag_y = relay(3, over_x, left, over_y)
    x_c = send(5, out_ref.at[over_x], out_ref.at[over_x], over_c)
    own_y.wait_recv()
    diag_x = relay(4, over_y, right, over_x)
    y_c = send(6, out_ref.at[over_y], out_ref.at[over_y], over_c)
    diag_y.wait_recv()
    left_c = relay(7, diag, left, over_c)
    diag_x.wait_recv()
    right_c = relay(8, diag, right, over_c)
    for copy in (own_c, x_c, y_c, left_c, right_c):
        copy.wait_recv()
    for copy in (own_x, own_y, own_c, diag_y, x_c, diag_x, y_c, left_c, right_c):
        copy.wait_send()


def gather_now(shard):
    rows, width = shard.shape
    out, token = pl.pallas_call(
        gather_kernel,
        in_specs=[pl.BlockSpec(memory_space=pltpu.VMEM)],
        out_specs=[pl.BlockSpec(memory_space=pltpu.VMEM)] * 2,
        out_shape=[jax.ShapeDtypeStruct((8, rows, width), shard.dtype), jax.ShapeDtypeStruct((8, 128), F32)],
        scratch_shapes=[pltpu.SemaphoreType.DMA((9,)), pltpu.SemaphoreType.DMA((9,))],
        compiler_params=pltpu.CompilerParams(collective_id=0, has_side_effects=True, vmem_limit_bytes=16 * 1024 * 1024),
        name='gather_attn0',
    )(shard)
    return out.reshape(8 * rows, width), token


def rms_forward(x, gain):
    inv = lax.rsqrt(jnp.mean(x * x, axis=0, keepdims=True) + NORM_EPS)
    return (x * inv * gain).astype(BF16), inv


def rms_backward(x, inv, gain, dn):
    dgain = jnp.sum(dn * (x * inv), axis=1)
    dxn = dn * gain
    dot = jnp.sum(dxn * x, axis=0, keepdims=True)
    return dxn * inv - x * (inv * inv * inv * dot * (1.0 / x.shape[0])), dgain


def core_half(a, core):
    rows = a.shape[0] // 8
    blocks = a.reshape(4, 2, rows, a.shape[1])
    return lax.dynamic_index_in_dim(blocks, core, axis=1, keepdims=False).reshape(4 * rows, a.shape[1])


def to_peer(part):
    return lax.ppermute(part, 'fsdp', CORE_SWAP)


def row_major(a):
    return with_layout_constraint(a, Layout(major_to_minor=tuple(range(a.ndim))))


def over_chips(part):
    return lax.psum_scatter(part, 'fsdp', scatter_dimension=0, tiled=True, axis_index_groups=SAME_CORE)


def tie(*values):
    return lax.optimization_barrier(values)


def gather(shard):
    return lax.all_gather(shard, 'fsdp', axis=0, tiled=True)


def solution(mesh):
    device_count = mesh.shape['dp'] * mesh.shape['fsdp']

    def local_step(hidden, cot_out, attn_norm, w_query, w_key, w_value, w_out, mlp_norm, w_gate, w_up, w_down):
        layers = attn_norm.shape[0]
        rows = attn_norm.shape[1]
        seq = hidden.shape[1]
        core = lax.rem(lax.axis_index('fsdp'), 2)
        cos, sin = rope_tables(seq, HD)
        grad_scale = 1.0 / (seq * device_count)
        gains = jnp.stack([attn_norm[0], mlp_norm[0], attn_norm[1], mlp_norm[1]], axis=1)
        gains = jnp.pad(gains, ((0, 0), (0, 124)))
        weights = []
        for l in range(layers):
            pieces = [w_query[l].reshape(rows, HEADS * HD), w_key[l].reshape(rows, KV * HD), w_value[l].reshape(rows, KV * HD), w_out[l]]
            if l == 0:
                pieces.append(gains)
            packed = jnp.concatenate(pieces, axis=1)
            if l:
                attn_w = gather(packed)
            else:
                attn_w, token = gather_now(packed)
            gate_up = gather(jnp.concatenate([w_gate[l], w_up[l]], axis=1))
            down = gather(w_down[l])
            if l == 0:
                token, w_query, w_key, w_value, w_out, w_gate, w_up, w_down = tie(token, w_query, w_key, w_value, w_out, w_gate, w_up, w_down)
            weights.append((attn_w, gate_up, down))
        gain_cols = weights[0][0][:, 2560:2564].astype(F32)
        x = hidden[0].T
        saved = []
        for l in range(layers):
            attn_w, gate_up, down = weights[l]
            g1, g2 = gain_cols[:, 2 * l:2 * l + 1], gain_cols[:, 2 * l + 1:2 * l + 2]
            xf = x.astype(F32)
            a, inv1 = rms_forward(xf, g1)
            qkv = dot_tn(attn_w[:, :1600], a)
            qr, kr, vb, o = attention_forward(qkv, cos, sin)
            x1 = (xf + dot_tn(attn_w[:, 1600:2560], o)).astype(BF16)
            x1f = x1.astype(F32)
            b, inv2 = rms_forward(x1f, g2)
            gate, up, act = mlp_forward(gate_up, b)
            saved.append((x, a, inv1, g1, qr, kr, vb, o, x1, b, inv2, g2, gate, up, act))
            x = (x1f + dot_tn(down, act)).astype(BF16)
        y = x
        grad = cot_out[0].T
        outs = [[None] * 3 for _ in range(layers)]
        gain_grads = [None] * (2 * layers)
        waiting, moving = [], []

        def release(value):
            l, slot, part = waiting.pop(0)
            if moving:
                done_l, done_slot, mine, peer = moving.pop(0)
                total = (mine + peer) * grad_scale
                value, part, outs[done_l][done_slot] = tie(value, part, total)
            else:
                value, part = tie(value, part)
            moving.append((l, slot, part, lax.ppermute(part, 'dp', DP_SWAP)))
            return value

        for l in reversed(range(layers)):
            attn_w, gate_up, down = weights[l]
            x, a, inv1, g1, qr, kr, vb, o, x1, b, inv2, g2, gate, up, act = saved[l]
            wide = jnp.pad(grad, ((0, 64), (0, 0)))
            other_down = row_major(dot_nt(core_half(act, 1 - core), wide))
            grad, other_down = tie(grad, other_down)
            sent_down = to_peer(other_down)
            act_mine = core_half(act, core)
            if l == 0:
                dgu = mlp_backward(down, grad, gate, up)
                act_mine, dgu = tie(act_mine, dgu)
                mine_down = row_major(dot_nt(act_mine, wide) + sent_down)
            else:
                mine_down = row_major(dot_nt(act_mine, wide) + sent_down)
                grad, mine_down = tie(grad, mine_down)
                dgu = mlp_backward(down, grad, gate, up)
            other_gu = row_major(dot_nt(core_half(b, 1 - core), dgu))
            if l == 0:
                dgu, mine_down, other_gu = tie(dgu, mine_down, other_gu)
            else:
                dgu, other_gu = tie(dgu, other_gu)
            waiting.append((l, 2, over_chips(mine_down)))
            sent_gu = to_peer(other_gu)
            db = dot_nn(gate_up, dgu).astype(BF16).astype(F32)
            dx1n, gain_grads[2 * l + 1] = rms_backward(x1.astype(F32), inv2, g2, db)
            dmid = (grad.astype(F32) + dx1n).astype(BF16)
            if l == 0:
                dmid = release(dmid)
            b_mine, dmid = tie(core_half(b, core), dmid)
            mine_gu = row_major(dot_nt(b_mine, dgu) + sent_gu)
            other_o = row_major(dot_nt(core_half(o, 1 - core), dmid))
            dmid, mine_gu, other_o = tie(dmid, mine_gu, other_o)
            waiting.append((l, 1, over_chips(mine_gu)))
            sent_o = to_peer(other_o)
            do = dot_nn(attn_w[:, 1600:2560], dmid).astype(BF16)
            dq, dk, dv = attention_backward(qr, kr, vb, do, cos, sin)
            dqkv = release(jnp.concatenate([dq, dk, dv], axis=0))
            o_mine, dqkv = tie(core_half(o, core), dqkv)
            mine_o = dot_nt(o_mine, dmid) + sent_o
            other_qkv = row_major(dot_nt(core_half(a, 1 - core), dqkv))
            dqkv, mine_o, other_qkv = tie(dqkv, mine_o, other_qkv)
            sent_qkv = to_peer(other_qkv)
            da = dot_nn(attn_w[:, :1600], dqkv).astype(BF16).astype(F32)
            dxn, gain_grads[2 * l] = rms_backward(x.astype(F32), inv1, g1, da)
            grad = (dmid.astype(F32) + dxn).astype(BF16)
            a_mine, grad = tie(core_half(a, core), grad)
            mine_qkv = dot_nt(a_mine, dqkv) + sent_qkv
            parts = [mine_qkv, mine_o]
            if l == 0:
                cols = jnp.pad(jnp.stack(gain_grads, axis=1), ((0, 0), (0, 124)))
                parts.append(core_half(cols, core) + to_peer(core_half(cols, 1 - core)))
            part = row_major(jnp.concatenate(parts, axis=1))
            grad, part = tie(grad, part)
            if l == 0:
                part = release(release(part))
            waiting.append((l, 0, over_chips(part)))
        (l, slot, part), = waiting
        moving.append((l, slot, part, lax.ppermute(part, 'dp', DP_SWAP)))
        for l, slot, mine, peer in moving:
            outs[l][slot] = (mine + peer) * grad_scale
        ra = [o[0] for o in outs]
        rg = [o[1] for o in outs]
        rd = [o[2][:, :D] for o in outs]
        gain = ra[0][:, 2560:2564]
        stack = lambda parts: jnp.stack(parts)
        return (
            y.T[None], grad.T[None],
            stack([gain[:, 0], gain[:, 2]]),
            stack([r[:, :960].reshape(rows, HEADS, HD) for r in ra]),
            stack([r[:, 960:1280].reshape(rows, KV, HD) for r in ra]),
            stack([r[:, 1280:1600].reshape(rows, KV, HD) for r in ra]),
            stack([r[:, 1600:2560] for r in ra]),
            stack([gain[:, 1], gain[:, 3]]),
            stack([r[:, :FF] for r in rg]),
            stack([r[:, FF:] for r in rg]),
            stack(rd),
        )

    return jax.shard_map(local_step, mesh=mesh, in_specs=(TOKEN_SPEC, TOKEN_SPEC) + WEIGHT_SPECS, out_specs=(TOKEN_SPEC, TOKEN_SPEC) + WEIGHT_SPECS, check_vma=False)
```

```python
import functools
import math
import jax
import jax.numpy as jnp
from jax import lax
from jax.experimental import pallas as pl
from jax.experimental.layout import Layout, with_layout_constraint
from jax.experimental.pallas import tpu as pltpu
from jax.sharding import PartitionSpec as P

NORM_EPS = 1e-5
ROPE_THETA = 500000.0
ROPE_FACTOR = 8.0
LOW_FACTOR = 1.0
HIGH_FACTOR = 4.0
OLD_CONTEXT = 8192.0
F32 = jnp.float32
BF16 = jnp.bfloat16
D, HEADS, KV, HD, FF = 960, 15, 5, 64, 2560
GROUP = HEADS // KV
BLK = 256
WEST = 1408
TOKEN_SPEC = P(('dp', 'fsdp'), None, None)
WEIGHT_SPECS = (P(None, 'fsdp'), P(None, 'fsdp', None, None), P(None, 'fsdp', None, None), P(None, 'fsdp', None, None), P(None, 'fsdp', None), P(None, 'fsdp'), P(None, 'fsdp', None), P(None, 'fsdp', None), P(None, 'fsdp', None))
CORE_SWAP = [(i, i ^ 1) for i in range(8)]
DP_SWAP = [(0, 1), (1, 0)]
SAME_CORE = [[0, 2, 4, 6], [1, 3, 5, 7]]
LOG2E = 1.4426950408889634
SCALE = HD ** -0.5


def rope_tables(seq_len, head_dim):
    half_dim = head_dim // 2
    base_freq = 1.0 / (ROPE_THETA ** (jnp.arange(half_dim, dtype=jnp.float32) * 2.0 / head_dim))
    wave_len = 2.0 * math.pi / base_freq
    smooth = (OLD_CONTEXT / wave_len - LOW_FACTOR) / (HIGH_FACTOR - LOW_FACTOR)
    mid_freq = (1.0 - smooth) * base_freq / ROPE_FACTOR + smooth * base_freq
    scaled_freq = jnp.where(wave_len < OLD_CONTEXT / HIGH_FACTOR, base_freq, jnp.where(wave_len > OLD_CONTEXT / LOW_FACTOR, base_freq / ROPE_FACTOR, mid_freq))
    angles = jnp.arange(seq_len, dtype=jnp.float32)[None, :] * scaled_freq[:, None]
    return jnp.cos(angles), jnp.sin(angles)


def dot_nn(a, b):
    return lax.dot_general(a, b, (((1,), (0,)), ((), ())), preferred_element_type=F32)


def dot_nt(a, b):
    return lax.dot_general(a, b, (((1,), (1,)), ((), ())), preferred_element_type=F32)


def dot_tn(a, b):
    return lax.dot_general(a, b, (((0,), (0,)), ((), ())), preferred_element_type=F32)


def rotate(x, cos, sin):
    u, w = x[:HD // 2], x[HD // 2:]
    return jnp.concatenate([u * cos - w * sin, w * cos + u * sin], axis=0)


def unrotate(x, cos, sin):
    u, w = x[:HD // 2], x[HD // 2:]
    return jnp.concatenate([u * cos + w * sin, w * cos - u * sin], axis=0)


def score_parts(k_ref, q, i):
    parts = []
    if i:
        parts.append(dot_nn(k_ref[:i * BLK], q))
    diag = dot_nn(k_ref[i * BLK:(i + 1) * BLK], q)
    keys = lax.broadcasted_iota(jnp.int32, (BLK, BLK), 0)
    queries = lax.broadcasted_iota(jnp.int32, (BLK, BLK), 1)
    parts.append(jnp.where(keys <= queries, diag, -1e30 / SCALE))
    return parts


def softmax_parts(parts):
    top = functools.reduce(jnp.maximum, [jnp.max(s, axis=0, keepdims=True) for s in parts])
    exps = [jnp.exp2((s - top) * (SCALE * LOG2E)) for s in parts]
    inv = 1.0 / sum(jnp.sum(e, axis=0, keepdims=True) for e in exps)
    return [e * inv for e in exps]


def attn_fwd_kernel(q_ref, k_ref, v_ref, cos_ref, sin_ref, qr_ref, kr_ref, vb_ref, o_ref, kt_ref):
    cos, sin = cos_ref[...], sin_ref[...]
    kr = rotate(k_ref[...], cos, sin).astype(BF16)
    kr_ref[...] = kr
    kt_ref[...] = jnp.transpose(kr.astype(F32)).astype(BF16)
    vb_ref[...] = v_ref[...].astype(BF16)

    def head(h, carry):
        rows = pl.ds(pl.multiple_of(h * HD, HD), HD)
        qr_ref[rows, :] = rotate(q_ref[rows, :], cos, sin).astype(BF16)
        for i in range(q_ref.shape[1] // BLK):
            cols = slice(i * BLK, (i + 1) * BLK)
            probs = softmax_parts(score_parts(kt_ref, qr_ref[rows, cols], i))
            base = 0
            out = None
            for p in probs:
                term = dot_nn(vb_ref[:, base:base + p.shape[0]], p.astype(BF16))
                out = term if out is None else out + term
                base += p.shape[0]
            o_ref[rows, cols] = out.astype(BF16)
        return carry

    lax.fori_loop(0, GROUP, head, 0)


def attn_bwd_kernel(q_ref, k_ref, v_ref, do_ref, cos_ref, sin_ref, dq_ref, dk_ref, dv_ref, kt_ref, vt_ref, dka_ref, dva_ref):
    cos, sin = cos_ref[...], sin_ref[...]
    kt_ref[...] = jnp.transpose(k_ref[...].astype(F32)).astype(BF16)
    vt_ref[...] = jnp.transpose(v_ref[...].astype(F32)).astype(BF16)
    dka_ref[...] = jnp.zeros_like(dka_ref)
    dva_ref[...] = jnp.zeros_like(dva_ref)

    def head(h, carry):
        rows = pl.ds(pl.multiple_of(h * HD, HD), HD)
        for i in range(q_ref.shape[1] // BLK):
            cols = slice(i * BLK, (i + 1) * BLK)
            q, do = q_ref[rows, cols], do_ref[rows, cols]
            probs = softmax_parts(score_parts(kt_ref, q, i))
            base = 0
            dps = []
            for p in probs:
                keys = slice(base, base + p.shape[0])
                dps.append(dot_nn(vt_ref[keys], do).astype(BF16).astype(F32))
                dva_ref[keys] += dot_nt(p.astype(BF16), do)
                base += p.shape[0]
            mean = sum(jnp.sum(p * dp, axis=0, keepdims=True) for p, dp in zip(probs, dps))
            base = 0
            dq = None
            for p, dp in zip(probs, dps):
                keys = slice(base, base + p.shape[0])
                ds = (p * (dp - mean)).astype(BF16)
                dka_ref[keys] += dot_nt(ds, q)
                term = dot_nn(k_ref[:, keys], ds)
                dq = term if dq is None else dq + term
                base += p.shape[0]
            dq = (dq * SCALE).astype(BF16).astype(F32)
            dq_ref[rows, cols] = unrotate(dq, cos[:, cols], sin[:, cols]).astype(BF16)
        return carry

    lax.fori_loop(0, GROUP, head, 0)
    dk = (jnp.transpose(dka_ref[...]) * SCALE).astype(BF16).astype(F32)
    dk_ref[...] = unrotate(dk, cos, sin).astype(BF16)
    dv_ref[...] = jnp.transpose(dva_ref[...]).astype(BF16)


def head_spec(seq, first, size):
    return pl.BlockSpec((size, seq), lambda g: (first + g, 0))


def attention_forward(qkv, cos, sin):
    seq = qkv.shape[1]
    full = pl.BlockSpec((HD // 2, seq), lambda g: (0, 0))
    shape = lambda rows: jax.ShapeDtypeStruct((rows, seq), BF16)
    return pl.pallas_call(
        attn_fwd_kernel,
        grid=(KV,),
        in_specs=[head_spec(seq, 0, GROUP * HD), head_spec(seq, HEADS, HD), head_spec(seq, HEADS + KV, HD), full, full],
        out_specs=[head_spec(seq, 0, GROUP * HD), head_spec(seq, 0, HD), head_spec(seq, 0, HD), head_spec(seq, 0, GROUP * HD)],
        out_shape=[shape(HEADS * HD), shape(KV * HD), shape(KV * HD), shape(HEADS * HD)],
        scratch_shapes=[pltpu.VMEM((seq, HD), BF16)],
        compiler_params=pltpu.CompilerParams(dimension_semantics=('arbitrary',), vmem_limit_bytes=48 * 1024 * 1024),
        cost_estimate=pl.CostEstimate(flops=20_000_000_000, bytes_accessed=14_000_000, transcendentals=10_000_000),
        name='attn_fwd',
    )(qkv, qkv, qkv, cos, sin)


def attention_backward(qr, kr, vb, do, cos, sin):
    seq = qr.shape[1]
    full = pl.BlockSpec((HD // 2, seq), lambda g: (0, 0))
    shape = lambda rows: jax.ShapeDtypeStruct((rows, seq), BF16)
    return pl.pallas_call(
        attn_bwd_kernel,
        grid=(KV,),
        in_specs=[head_spec(seq, 0, GROUP * HD), head_spec(seq, 0, HD), head_spec(seq, 0, HD), head_spec(seq, 0, GROUP * HD), full, full],
        out_specs=[head_spec(seq, 0, GROUP * HD), head_spec(seq, 0, HD), head_spec(seq, 0, HD)],
        out_shape=[shape(HEADS * HD), shape(KV * HD), shape(KV * HD)],
        scratch_shapes=[pltpu.VMEM((seq, HD), BF16), pltpu.VMEM((seq, HD), BF16), pltpu.VMEM((seq, HD), F32), pltpu.VMEM((seq, HD), F32)],
        compiler_params=pltpu.CompilerParams(dimension_semantics=('arbitrary',), vmem_limit_bytes=48 * 1024 * 1024),
        cost_estimate=pl.CostEstimate(flops=40_000_000_000, bytes_accessed=14_000_000, transcendentals=10_000_000),
        name='attn_bwd',
    )(qr, kr, vb, do, cos, sin)


def mlp_fwd_kernel(b_ref, wg_ref, wu_ref, gate_ref, up_ref, act_ref):
    gate = dot_tn(wg_ref[...], b_ref[...])
    up = dot_tn(wu_ref[...], b_ref[...])
    gate_ref[...] = gate
    up_ref[...] = up
    act_ref[...] = (gate * jax.nn.sigmoid(gate) * up).astype(BF16)


def mlp_forward(gate_up, b):
    seq = b.shape[1]
    steps = FF // 256
    rows = pl.BlockSpec((256, seq), lambda i: (i, 0))
    wide = jax.ShapeDtypeStruct((FF, seq), F32)
    return pl.pallas_call(
        mlp_fwd_kernel,
        grid=(steps,),
        in_specs=[pl.BlockSpec((D, seq), lambda i: (0, 0)), pl.BlockSpec((D, 256), lambda i: (0, i)), pl.BlockSpec((D, 256), lambda i: (0, steps + i))],
        out_specs=[rows, rows, rows],
        out_shape=[wide, wide, jax.ShapeDtypeStruct((FF, seq), BF16)],
        compiler_params=pltpu.CompilerParams(dimension_semantics=('arbitrary',), vmem_limit_bytes=60 * 1024 * 1024),
        cost_estimate=pl.CostEstimate(flops=10_000_000_000, bytes_accessed=38_000_000, transcendentals=5_000_000),
        name='mlp_fwd',
    )(b, gate_up, gate_up)


def mlp_bwd_kernel(down_ref, grad_ref, gate_ref, up_ref, out_ref):
    dact = dot_nn(down_ref[...], grad_ref[...]).astype(BF16).astype(F32)
    gate, up = gate_ref[...], up_ref[...]
    sig = jax.nn.sigmoid(gate)
    out_ref[0] = (dact * up * (sig * (1.0 + gate * (1.0 - sig)))).astype(BF16)
    out_ref[1] = (dact * (gate * sig)).astype(BF16)


def mlp_backward(down, grad, gate, up):
    seq = grad.shape[1]
    rows = pl.BlockSpec((256, seq), lambda i: (i, 0))
    out = pl.pallas_call(
        mlp_bwd_kernel,
        grid=(FF // 256,),
        in_specs=[pl.BlockSpec((256, D), lambda i: (i, 0)), pl.BlockSpec((D, seq), lambda i: (0, 0)), rows, rows],
        out_specs=pl.BlockSpec((2, 256, seq), lambda i: (0, i, 0)),
        out_shape=jax.ShapeDtypeStruct((2, FF, seq), BF16),
        compiler_params=pltpu.CompilerParams(dimension_semantics=('arbitrary',), vmem_limit_bytes=32 * 1024 * 1024),
        cost_estimate=pl.CostEstimate(flops=5_000_000_000, bytes_accessed=38_000_000, transcendentals=5_000_000),
        name='mlp_bwd',
    )(down, grad, gate, up)
    return out.reshape(2 * FF, seq)


def merge_kernel(a_ref, g_ref, sent_ref, keep_ref, recv_ref, out_ref):
    step = pl.program_id(0)

    @pl.when(step < 4)
    def _():
        out_ref[...] = dot_nt(a_ref[...], g_ref[...]) + sent_ref[...]

    @pl.when(step == 4)
    def _():
        out_ref[...] = keep_ref[...] + recv_ref[...]


def merged_grad(a, g, sent, keep, recv):
    rows, seq = a.shape
    wide = keep.shape[1]
    whole = pl.BlockSpec((rows, wide), lambda j: (0, 0))
    return pl.pallas_call(
        merge_kernel,
        grid=(5,),
        in_specs=[pl.BlockSpec((rows, seq), lambda j: (0, 0)), pl.BlockSpec((wide, seq), lambda j: (jnp.minimum(j, 3), 0)),
                  pl.BlockSpec((rows, wide), lambda j: (0, jnp.minimum(j, 3))), whole, whole],
        out_specs=pl.BlockSpec((rows, wide), lambda j: (0, j)),
        out_shape=jax.ShapeDtypeStruct((rows, 5 * wide), F32),
        compiler_params=pltpu.CompilerParams(dimension_semantics=('arbitrary',), vmem_limit_bytes=48 * 1024 * 1024),
        cost_estimate=pl.CostEstimate(flops=5_000_000_000, bytes_accessed=40_000_000, transcendentals=0),
        name='merged_grad',
    )(a, g, sent, keep, recv)


def gather_kernel(shard_ref, out_ref, token_ref, send_sem, recv_sem):
    me = lax.axis_index('fsdp')
    over_c = me + 1 - 2 * (me % 2)
    over_x = me + 2 - 4 * ((me // 2) % 2)
    over_y = me + 4 - 8 * (me // 4)
    diag = over_x + over_y - me
    barrier = pltpu.get_barrier_semaphore()
    for peer in (over_x, over_y, over_c):
        pl.semaphore_signal(barrier, inc=1, device_id={'fsdp': peer}, device_id_type=pl.DeviceIdType.MESH)
    pl.semaphore_wait(barrier, 3)
    width = shard_ref.shape[1]
    left, right = pl.ds(0, WEST), pl.ds(WEST, width - WEST)

    def send(slot, src, dst, peer):
        copy = pltpu.make_async_remote_copy(
            src_ref=src, dst_ref=dst, send_sem=send_sem.at[slot], recv_sem=recv_sem.at[slot],
            device_id={'fsdp': peer}, device_id_type=pl.DeviceIdType.MESH)
        copy.start()
        return copy

    def relay(slot, shard, cols, peer):
        part = out_ref.at[shard, :, cols]
        return send(slot, part, part, peer)

    own_x = send(0, shard_ref, out_ref.at[me], over_x)
    own_y = send(1, shard_ref, out_ref.at[me], over_y)
    own_c = send(2, shard_ref, out_ref.at[me], over_c)
    out_ref[me] = shard_ref[...]
    token_ref[...] = jnp.zeros_like(token_ref)
    own_x.wait_recv()
    diag_y = relay(3, over_x, left, over_y)
    x_c = send(5, out_ref.at[over_x], out_ref.at[over_x], over_c)
    own_y.wait_recv()
    diag_x = relay(4, over_y, right, over_x)
    y_c = send(6, out_ref.at[over_y], out_ref.at[over_y], over_c)
    diag_y.wait_recv()
    left_c = relay(7, diag, left, over_c)
    diag_x.wait_recv()
    right_c = relay(8, diag, right, over_c)
    for copy in (own_c, x_c, y_c, left_c, right_c):
        copy.wait_recv()
    for copy in (own_x, own_y, own_c, diag_y, x_c, diag_x, y_c, left_c, right_c):
        copy.wait_send()


def gather_now(shard):
    rows, width = shard.shape
    out, token = pl.pallas_call(
        gather_kernel,
        in_specs=[pl.BlockSpec(memory_space=pltpu.VMEM)],
        out_specs=[pl.BlockSpec(memory_space=pltpu.VMEM)] * 2,
        out_shape=[jax.ShapeDtypeStruct((8, rows, width), shard.dtype), jax.ShapeDtypeStruct((8, 128), F32)],
        scratch_shapes=[pltpu.SemaphoreType.DMA((9,)), pltpu.SemaphoreType.DMA((9,))],
        compiler_params=pltpu.CompilerParams(collective_id=0, has_side_effects=True, vmem_limit_bytes=16 * 1024 * 1024),
        name='gather_attn0',
    )(shard)
    return out.reshape(8 * rows, width), token


def rms_forward(x, gain):
    inv = lax.rsqrt(jnp.mean(x * x, axis=0, keepdims=True) + NORM_EPS)
    return (x * inv * gain).astype(BF16), inv


def rms_backward(x, inv, gain, dn):
    dgain = jnp.sum(dn * (x * inv), axis=1)
    dxn = dn * gain
    dot = jnp.sum(dxn * x, axis=0, keepdims=True)
    return dxn * inv - x * (inv * inv * inv * dot * (1.0 / x.shape[0])), dgain


def core_half(a, core):
    rows = a.shape[0] // 8
    blocks = a.reshape(4, 2, rows, a.shape[1])
    return lax.dynamic_index_in_dim(blocks, core, axis=1, keepdims=False).reshape(4 * rows, a.shape[1])


def to_peer(part):
    return lax.ppermute(part, 'fsdp', CORE_SWAP)


def row_major(a):
    return with_layout_constraint(a, Layout(major_to_minor=tuple(range(a.ndim))))


def over_chips(part):
    return lax.psum_scatter(part, 'fsdp', scatter_dimension=0, tiled=True, axis_index_groups=SAME_CORE)


def tie(*values):
    return lax.optimization_barrier(values)


def gather(shard):
    return lax.all_gather(shard, 'fsdp', axis=0, tiled=True)


def solution(mesh):
    device_count = mesh.shape['dp'] * mesh.shape['fsdp']

    def local_step(hidden, cot_out, attn_norm, w_query, w_key, w_value, w_out, mlp_norm, w_gate, w_up, w_down):
        layers = attn_norm.shape[0]
        rows = attn_norm.shape[1]
        seq = hidden.shape[1]
        core = lax.rem(lax.axis_index('fsdp'), 2)
        cos, sin = rope_tables(seq, HD)
        grad_scale = 1.0 / (seq * device_count)
        gains = jnp.stack([attn_norm[0], mlp_norm[0], attn_norm[1], mlp_norm[1]], axis=1)
        gains = jnp.pad(gains, ((0, 0), (0, 124)))
        weights = []
        for l in range(layers):
            pieces = [w_query[l].reshape(rows, HEADS * HD), w_key[l].reshape(rows, KV * HD), w_value[l].reshape(rows, KV * HD), w_out[l]]
            if l == 0:
                pieces.append(gains)
            packed = jnp.concatenate(pieces, axis=1)
            if l:
                attn_w = gather(packed)
            else:
                attn_w, token = gather_now(packed)
            gate_up = gather(jnp.concatenate([w_gate[l], w_up[l]], axis=1))
            down = gather(w_down[l])
            if l == 0:
                token, w_query, w_key, w_value, w_out, w_gate, w_up, w_down = tie(token, w_query, w_key, w_value, w_out, w_gate, w_up, w_down)
            weights.append((attn_w, gate_up, down))
        gain_cols = weights[0][0][:, 2560:2564].astype(F32)
        x = hidden[0].T
        saved = []
        for l in range(layers):
            attn_w, gate_up, down = weights[l]
            g1, g2 = gain_cols[:, 2 * l:2 * l + 1], gain_cols[:, 2 * l + 1:2 * l + 2]
            xf = x.astype(F32)
            a, inv1 = rms_forward(xf, g1)
            qkv = dot_tn(attn_w[:, :1600], a)
            qr, kr, vb, o = attention_forward(qkv, cos, sin)
            x1 = (xf + dot_tn(attn_w[:, 1600:2560], o)).astype(BF16)
            x1f = x1.astype(F32)
            b, inv2 = rms_forward(x1f, g2)
            gate, up, act = mlp_forward(gate_up, b)
            saved.append((x, a, inv1, g1, qr, kr, vb, o, x1, b, inv2, g2, gate, up, act))
            x = (x1f + dot_tn(down, act)).astype(BF16)
        y = x
        grad = cot_out[0].T
        outs = [[None] * 3 for _ in range(layers)]
        gain_grads = [None] * (2 * layers)
        waiting, moving = [], []

        def release(value):
            l, slot, part = waiting.pop(0)
            if moving:
                done_l, done_slot, mine, peer = moving.pop(0)
                total = row_major((mine + row_major(peer)) * grad_scale)
                value, part, outs[done_l][done_slot] = tie(value, part, total)
            else:
                value, part = tie(value, part)
            moving.append((l, slot, part, lax.ppermute(part, 'dp', DP_SWAP)))
            return value

        for l in reversed(range(layers)):
            attn_w, gate_up, down = weights[l]
            x, a, inv1, g1, qr, kr, vb, o, x1, b, inv2, g2, gate, up, act = saved[l]
            wide = jnp.pad(grad, ((0, 64), (0, 0)))
            other_down = row_major(dot_nt(core_half(act, 1 - core), wide))
            grad, other_down = tie(grad, other_down)
            sent_down = to_peer(other_down)
            act_mine = core_half(act, core)
            if l == 0:
                dgu = mlp_backward(down, grad, gate, up)
                act_mine, dgu = tie(act_mine, dgu)
                mine_down = row_major(dot_nt(act_mine, wide) + sent_down)
            else:
                mine_down = row_major(dot_nt(act_mine, wide) + sent_down)
                grad, mine_down = tie(grad, mine_down)
                dgu = mlp_backward(down, grad, gate, up)
            other_gu = row_major(dot_nt(core_half(b, 1 - core), dgu))
            if l == 0:
                dgu, mine_down, other_gu = tie(dgu, mine_down, other_gu)
            else:
                dgu, other_gu = tie(dgu, other_gu)
            waiting.append((l, 2, over_chips(mine_down)))
            sent_gu = to_peer(other_gu)
            db = dot_nn(gate_up, dgu).astype(BF16).astype(F32)
            dx1n, gain_grads[2 * l + 1] = rms_backward(x1.astype(F32), inv2, g2, db)
            dmid = (grad.astype(F32) + dx1n).astype(BF16)
            if l == 0:
                dmid = release(dmid)
            b_mine, dmid = tie(core_half(b, core), dmid)
            if l == 0:
                mine_gu = merged_grad(b_mine, dgu, sent_gu, *late_attn)
            else:
                mine_gu = row_major(dot_nt(b_mine, dgu) + sent_gu)
            other_o = row_major(dot_nt(core_half(o, 1 - core), dmid))
            dmid, mine_gu, other_o = tie(dmid, mine_gu, other_o)
            waiting.append((l, 1, over_chips(mine_gu)))
            sent_o = to_peer(other_o)
            do = dot_nn(attn_w[:, 1600:2560], dmid).astype(BF16)
            dq, dk, dv = attention_backward(qr, kr, vb, do, cos, sin)
            dqkv = release(jnp.concatenate([dq, dk, dv], axis=0))
            o_mine, dqkv = tie(core_half(o, core), dqkv)
            mine_o = dot_nt(o_mine, dmid) + sent_o
            other_qkv = row_major(dot_nt(core_half(a, 1 - core), dqkv))
            dqkv, mine_o, other_qkv = tie(dqkv, mine_o, other_qkv)
            sent_qkv = to_peer(other_qkv)
            da = dot_nn(attn_w[:, :1600], dqkv).astype(BF16).astype(F32)
            dxn, gain_grads[2 * l] = rms_backward(x.astype(F32), inv1, g1, da)
            grad = (dmid.astype(F32) + dxn).astype(BF16)
            a_mine, grad = tie(core_half(a, core), grad)
            mine_qkv = dot_nt(a_mine, dqkv) + sent_qkv
            parts = [mine_qkv, mine_o]
            if l == 0:
                cols = jnp.pad(jnp.stack(gain_grads, axis=1), ((0, 0), (0, 124)))
                parts.append(core_half(cols, core) + to_peer(core_half(cols, 1 - core)))
            part = row_major(jnp.concatenate(parts, axis=1))
            grad, part = tie(grad, part)
            if l == 0:
                part = release(part)
                waiting.append((l, 0, over_chips(part)))
            else:
                low = lax.axis_index('dp') == 0
                left, right = part[:, :1280], part[:, 1280:]
                other = lax.ppermute(jnp.where(low, right, left), 'dp', DP_SWAP)
                late_attn = (jnp.where(low, left, right), other)
        (l, slot, part), = waiting
        moving.append((l, slot, part, lax.ppermute(part, 'dp', DP_SWAP)))
        (_, _, mine, peer), (_, _, last, last_peer) = moving
        mine, peer = row_major(mine), row_major(peer)
        rg0 = row_major((mine[:, :2 * FF] + peer[:, :2 * FF]) * grad_scale)
        mine, peer = mine[:, 2 * FF:] * grad_scale, peer[:, 2 * FF:] * grad_scale
        first = row_major(jnp.where(low, mine, peer))
        second = row_major(jnp.where(low, peer, mine))
        ra = row_major((row_major(last) + row_major(last_peer)) * grad_scale)
        rg = outs[1][1]
        rd = [o[2][:, :D] for o in outs]
        gain = ra[:, 2560:2564]
        stack = lambda parts: jnp.stack(parts)
        return (
            y.T[None], grad.T[None],
            stack([gain[:, 0], gain[:, 2]]),
            stack([ra[:, :960].reshape(rows, HEADS, HD), first[:, :960].reshape(rows, HEADS, HD)]),
            stack([ra[:, 960:1280].reshape(rows, KV, HD), first[:, 960:].reshape(rows, KV, HD)]),
            stack([ra[:, 1280:1600].reshape(rows, KV, HD), second[:, :320].reshape(rows, KV, HD)]),
            stack([ra[:, 1600:2560], second[:, 320:]]),
            stack([gain[:, 1], gain[:, 3]]),
            stack([rg0[:, :FF], rg[:, :FF]]),
            stack([rg0[:, FF:], rg[:, FF:]]),
            stack(rd),
        )

    return jax.shard_map(local_step, mesh=mesh, in_specs=(TOKEN_SPEC, TOKEN_SPEC) + WEIGHT_SPECS, out_specs=(TOKEN_SPEC, TOKEN_SPEC) + WEIGHT_SPECS, check_vma=False)
```
